32 devices in a mesh: row: 8 (over z, y), col: 4 (over x, core).
Axes of the slice: x: 2, y: 2, z: 4, core: 2. Of those that a mesh axis runs over, the one named last changes fastest.
Arguments:
- tokens: bfloat16 [4096, 4096], P('row', 'col'), may hold values from -6 to 6
- norm_gain: bfloat16 [4096], P('col'), may hold values from 0.099609375 to 1.8984375
- gate_weight: bfloat16 [4096, 10240], P('row', 'col'), may hold values from -0.09375 to 0.09375
- linear_weight: bfloat16 [4096, 10240], P('row', 'col'), may hold values from -0.09375 to 0.09375
- output_weight: bfloat16 [10240, 4096], P('col', 'row'), may hold values from -0.078125 to 0.078125
Outputs:
- block_out: bfloat16 [4096, 4096], P('row', 'col')
The draws below stay inside these ranges and needn't reach their ends.
All inputs are finite; a program needn't handle non-finite values.
Results may differ from the reference program's by a relative error of at most 0.0065.
Values may be sent and summed in bfloat16 or wider, within the bound.
A program may use at most 128 MiB of HBM per device.

```python
import jax
import jax.numpy as jnp
from jax import lax

D = 4096
FF = 10240
TOKENS = 4096


def raised(entries, key, source, target, shards_of, factor):
    owner, partner = [(jnp.arange(entries.shape[dim]) // (entries.shape[dim] // shards_of)).reshape([-1 if axis == dim else 1 for axis in range(entries.ndim)]) for dim in (source, target)]
    chosen = jax.random.permutation(key, shards_of)[partner]
    strong = (owner == chosen) | (owner == (partner + shards_of // 2) % shards_of)
    return jnp.where(strong, factor * entries, entries)


def steps_of(key, dims, pieces, low, high):
    def one(axis_at, shards_of):
        heights = jax.random.uniform(jax.random.fold_in(jax.random.fold_in(key, 6), axis_at), (shards_of,), jnp.float32, low / len(pieces), high / len(pieces))
        return jnp.repeat(jnp.exp(heights), dims[axis_at] // shards_of).reshape((-1,) + (1,) * (len(dims) - axis_at - 1))

    gain = one(*pieces[0])
    for cut in pieces[1:]:
        gain = gain * one(*cut)
    return gain


def scatter_about(key, shape, deviation, reach, pieces=(), dtype=jnp.bfloat16):
    array = deviation * jax.random.normal(key, shape, jnp.float32)
    if pieces:
        array = array * steps_of(key, shape, pieces, -0.22, 0.18)
    return jnp.clip(array, -reach, reach).astype(dtype)


def noise_with(rng, dims, width, bound, pieces, heavy, kind=jnp.bfloat16):
    result = width * jax.random.normal(rng, dims, jnp.float32)
    if pieces:
        result = result * steps_of(rng, dims, pieces, -0.22, 0.18)
    return jnp.clip(raised(result, jax.random.fold_in(rng, 3), *heavy), -bound, bound).astype(kind)


def setup_inputs(seed: int = 0) -> dict:
    key_of = jax.random.split(jax.random.key(seed), 6)
    return {
        "tokens": scatter_about(key_of[0], (TOKENS, D), 1.0, 6.0, ((0, 8), (1, 4))),
        "norm_gain": jnp.clip(1.0 + 0.18 * jax.random.normal(key_of[1], (D,), jnp.float32), 0.099609375, 1.8984375).astype(jnp.bfloat16),
        "gate_weight": scatter_about(key_of[2], (D, FF), D ** -0.5, 0.09375, ((0, 8), (1, 4))),
        "linear_weight": scatter_about(key_of[3], (D, FF), D ** -0.5, 0.09375, ((0, 8), (1, 4))),
        "output_weight": noise_with(key_of[4], (FF, D), FF ** -0.5, 0.078125, ((0, 4), (1, 8)), (0, 1, 8, 2.0)),
    }


def reference(tokens, norm_gain, gate_weight, linear_weight, output_weight):
    values = tokens.astype(jnp.float32)
    meansq = lax.optimization_barrier(jnp.mean(values * values, axis=-1, keepdims=True))
    normed = (values * jax.lax.rsqrt(meansq + 1e-06) * norm_gain.astype(jnp.float32)).astype(jnp.bfloat16)
    gate = jnp.dot(normed, gate_weight, preferred_element_type=jnp.float32)
    linear = jnp.dot(normed, linear_weight, preferred_element_type=jnp.float32)
    hidden = (jax.nn.gelu(gate, approximate=True) * linear).astype(jnp.bfloat16)
    return jnp.dot(hidden, output_weight, preferred_element_type=jnp.float32).astype(jnp.bfloat16)
```

```python
import functools

import jax
import jax.numpy as jnp
from jax import lax
from jax.experimental import pallas as pl
from jax.experimental.pallas import tpu as pltpu
from jax.sharding import PartitionSpec as P

LANES = 128
VMEM_LIMIT = 67043328
SCRATCH_MOST = 61 << 20
MESH = pl.DeviceIdType.MESH
F32 = jnp.float32
BF16 = jnp.bfloat16


def gathered(tokens, norm_gain, gate_weight, linear_weight, output_weight):
    whole = lax.all_gather(tokens, "col", axis=1, tiled=True)
    gain_all = lax.all_gather(norm_gain, "col", axis=0, tiled=True)
    normed = rms_normed(whole, gain_all)
    gate = dot(normed, lax.all_gather(gate_weight, "row", axis=0, tiled=True))
    linear = dot(normed, lax.all_gather(linear_weight, "row", axis=0, tiled=True))
    hidden = (jax.nn.gelu(gate, approximate=True) * linear).astype(BF16)
    terms = dot(hidden, lax.all_gather(output_weight, "row", axis=1, tiled=True))
    return lax.psum_scatter(terms, "col", scatter_dimension=1, tiled=True).astype(BF16)


def dot(left, right):
    return jnp.dot(left, right, preferred_element_type=F32)


def rms_normed(whole, gain_all):
    values = whole.astype(F32)
    meansq = jnp.mean(values * values, axis=-1, keepdims=True)
    return (values * lax.rsqrt(meansq + 1e-06) * gain_all.astype(F32)).astype(BF16)


def pick(index, table):
    value = jnp.int32(table[0])
    for at in range(1, len(table)):
        value = jnp.where(index == at, jnp.int32(table[at]), value)
    return value


def body(zs, tokens, gain, gate_w, linear_w, out_w, out, xn, gl, acc, hid, wo, ss, *sems):
    (loc, ss_s, ss_r, t_r, t_zr, t_zl, t_x, t_c, t_d, g_z, g_y, g_zs, g_ys, w_z, w_zs, w_x, w_xs,
     w_y, w_ys, h_r, h_x, h_c, h_d, o_r, o_s, credit) = sems
    size, width = tokens.shape
    part = hid.shape[2] // zs
    outw = out_w.shape[1]
    features = width * zs
    row, col = lax.axis_index("row"), lax.axis_index("col")
    z, y = row // 2, row % 2
    x, core = col // 2, col % 2
    xcol = (1 - x) * 2 + core
    ccol = x * 2 + 1 - core
    dcol = (1 - x) * 2 + 1 - core
    near = [z, z + 1 - 2 * (z % 2), zs - 1 - z, (z + 2) % zs]
    at_x, at_c, at_d = (row, xcol), (row, ccol), (row, dcol)
    at_y = (z * 2 + 1 - y, col)

    def at_z(to):
        return (to * 2 + y, col)

    def copy(src, dst, send, recv, to):
        return pltpu.make_async_remote_copy(
            src_ref=src, dst_ref=dst, send_sem=send, recv_sem=recv, device_id=to, device_id_type=MESH
        )

    def arrived(ref, sem):
        copy(ref, ref, sem, sem, at_c).wait_recv()

    def left_here(ref, sem):
        copy(ref, ref, sem, sem, at_c).wait_send()

    def gl_at(zz, yy, i):
        return gl.at[zz, yy, :, pl.ds(i * part, part)]

    def wo_at(slab, block):
        return wo.at[slab, pl.ds(pl.multiple_of(block * part, 128), part), :]

    def hid_at(b, k):
        return hid.at[b, :, pl.ds(pl.multiple_of(k * part, 128), part)]

    def cols_of(w, to):
        return w.at[:, pl.ds(pl.multiple_of(to * part, 128), part)]

    own = xn.at[col, z]
    w_slab, w_block = jnp.where(z == col, y, 2), jnp.where(z == col, col, z)
    ins = [
        pltpu.make_async_copy(tokens, own, loc.at[0]),
        pltpu.make_async_copy(cols_of(gate_w, z), gl_at(z, y, 0), loc.at[1]),
        pltpu.make_async_copy(cols_of(linear_w, z), gl_at(z, y, 1), loc.at[2]),
        pltpu.make_async_copy(
            out_w.at[pl.ds(pl.multiple_of(z * part, 128), part), :], wo_at(w_slab, w_block), loc.at[3]
        ),
    ]
    for each in ins:
        each.start()

    barrier = pltpu.get_barrier_semaphore()
    peers = [at_z(near[1]), at_z(near[2]), at_z(near[3]), at_y, at_x, at_c, at_d]
    for peer in peers:
        pl.semaphore_signal(barrier, inc=1, device_id=peer, device_id_type=MESH)

    ins[0].wait()
    piece = 64

    @pl.loop(0, size // piece)
    def _(i):
        rows = pl.ds(pl.multiple_of(i * piece, piece), piece)
        values = xn[col, z, rows, :].astype(F32)
        sums = jnp.sum(values * values, axis=-1, keepdims=True)
        ss[col, rows, :] = jnp.broadcast_to(sums, (piece, LANES))

    pl.semaphore_wait(barrier, len(peers))

    def g_send(m, i):
        to = near[m]
        copy(
            cols_of((gate_w, linear_w)[i], to), gl_at(z, y, i), g_zs.at[m, i], g_z.at[z, i], at_z(to)
        ).start()

    def g_pass(m, i):
        ref = gl_at(near[m], y, i)
        copy(ref, ref, g_ys.at[m, i], g_y.at[near[m], i], at_y).start()

    def g_took(m, i):
        arrived(gl_at(near[m], y, i), g_z.at[near[m], i])
        g_pass(m, i)

    g_send(2, 0)
    for n, peer in enumerate((at_x, at_c, at_d)):
        copy(ss.at[col], ss.at[col], ss_s.at[n], ss_r.at[col], peer).start()
    ins[1].wait()
    g_pass(0, 0)
    ins[2].wait()
    g_pass(0, 1)
    for k in (xcol, ccol, dcol):
        arrived(ss.at[k], ss_r.at[k])

    @pl.loop(0, size // piece)
    def _(i):
        rows = pl.ds(pl.multiple_of(i * piece, piece), piece)
        total = ss[0, rows, :]
        for k in range(1, zs):
            total = total + ss[k, rows, :]
        scale = lax.rsqrt(total * (1.0 / features) + 1e-06)
        scale = jnp.concatenate([scale] * (width // LANES), axis=1)
        values = xn[col, z, rows, :].astype(F32) * scale * gain[...].astype(F32)
        xn[col, z, rows, :] = values.astype(BF16)

    def t_right(b):
        copy(xn.at[col, b], xn.at[col, b], t_zr.at[b], t_r.at[col, b], at_z(z + 1)).start()

    def t_left(b):
        copy(xn.at[col, b], xn.at[col, b], t_zl.at[b], t_r.at[col, b], at_z(z - 1)).start()

    def t_col(b):
        copy(xn.at[col, b], xn.at[col, b], t_x.at[b], t_r.at[col, b], at_x).start()
        copy(xn.at[col, b], xn.at[col, b], t_c.at[b], t_r.at[col, b], at_c).start()

    def t_over(b):
        arrived(xn.at[xcol, b], t_r.at[xcol, b])
        copy(xn.at[xcol, b], xn.at[xcol, b], t_d.at[b], t_r.at[xcol, b], at_c).start()

    pl.when(z < zs - 1)(lambda: t_right(z))
    pl.when(z > 0)(lambda: t_left(z))
    t_col(z)
    g_send(1, 0)
    g_send(1, 1)

    def w_out(m):
        zz = near[m]
        slab, block = jnp.where(zz == col, y, 2), jnp.where(zz == col, col, zz)
        ref = wo_at(slab, block)

        @pl.when(zz == col)
        def _():
            copy(ref, ref, w_ys.at[col], w_y.at[col], at_y).start()

        @pl.when(zz != col)
        def _():
            copy(ref, wo_at(y, col), w_xs.at[m], w_x.at[col], (row, zz)).start()

    def w_send(m):
        to = near[m]
        copy(
            out_w.at[pl.ds(pl.multiple_of(to * part, 128), part), :],
            wo_at(w_slab, w_block), w_zs.at[m], w_z.at[z], at_z(to),
        ).start()

    def w_took(m):
        zz = near[m]
        slab, block = jnp.where(zz == col, y, 2), jnp.where(zz == col, col, zz)
        arrived(wo_at(slab, block), w_z.at[zz])
        w_out(m)

    ins[3].wait()
    w_out(0)

    def t_step(s):
        @pl.when(z >= s)
        def _():
            b = z - s
            arrived(xn.at[col, b], t_r.at[col, b])
            pl.when(z < zs - 1)(lambda: t_right(b))
            t_col(b)

        @pl.when(z + s < zs)
        def _():
            b = z + s
            arrived(xn.at[col, b], t_r.at[col, b])
            pl.when(z > 0)(lambda: t_left(b))
            t_col(b)

    def t_over_step(s):
        pl.when(z >= s)(lambda: t_over(z - s))
        pl.when(z + s < zs)(lambda: t_over(z + s))

    t_step(1)
    g_send(2, 1)
    g_send(3, 0)
    t_over(z)
    t_step(2)
    g_send(3, 1)
    t_over_step(1)
    t_step(3)
    for m in (2, 3, 1):
        w_send(m)
    t_over_step(2)
    g_took(1, 0)
    g_took(1, 1)
    t_over_step(3)
    g_took(2, 0)

    tile = 2 * LANES
    tiles = 2 * part // tile
    depth = gl.shape[2]

    def product(kk, b, n):
        lanes = pl.ds(pl.multiple_of(n * tile, tile), tile)
        return dot(xn[kk, b, :, :depth], gl[kk, 0, :, lanes]) + dot(
            xn[kk, b, :, depth:], gl[kk, 1, :, lanes]
        ), lanes

    def inputs(m, first):
        kk = near[m]
        if first:
            for b in range(zs):
                for k in (ccol, dcol):
                    arrived(xn.at[k, b], t_r.at[k, b])
        for i in range(2):
            arrived(gl_at(kk, 1 - y, i), g_y.at[kk, i])

        @pl.loop(0, zs * tiles)
        def _(i):
            b, n = i // tiles, i % tiles
            value, lanes = product(kk, b, n)
            if first:
                acc[b, :, lanes] = value
            else:
                acc[b, :, lanes] = acc[b, :, lanes] + value

    inputs(0, True)
    g_took(2, 1)
    inputs(1, False)
    g_took(3, 0)
    g_took(3, 1)
    inputs(2, False)

    orders = [sorted(range(zs), key=lambda b, at=at: -abs(b - at)) for at in range(zs)]
    blocks = [pick(z, [order[j] for order in orders]) for j in range(zs)]

    last = near[3]
    for i in range(2):
        arrived(gl_at(last, 1 - y, i), g_y.at[last, i])
    cut = 64

    for j in range(zs):
        b = blocks[j]

        @pl.loop(0, tiles)
        def _(n, b=b):
            value, lanes = product(last, b, n)
            acc[b, :, lanes] = acc[b, :, lanes] + value

        @pl.loop(0, size // cut)
        def _(i, b=b):
            rows = pl.ds(pl.multiple_of(i * cut, cut), cut)
            gate = acc[b, rows, :part]
            linear = acc[b, rows, part:]
            value = (jax.nn.gelu(gate, approximate=True) * linear).astype(BF16)
            hid[b, rows, pl.ds(pl.multiple_of(col * part, 128), part)] = value

        copy(hid_at(b, col), hid_at(b, col), h_x.at[j], h_r.at[col, b], at_x).start()
        copy(hid_at(b, col), hid_at(b, col), h_c.at[j], h_r.at[col, b], at_c).start()

    def h_over(j):
        b = blocks[j]
        arrived(hid_at(b, xcol), h_r.at[xcol, b])
        copy(hid_at(b, xcol), hid_at(b, xcol), h_d.at[j], h_r.at[xcol, b], at_c).start()

    for b in range(zs):
        left_here(xn.at[col, b], t_x.at[b])
        left_here(xn.at[col, b], t_c.at[b])
        left_here(xn.at[xcol, b], t_d.at[b])

        @pl.when((b <= z) & (z < zs - 1))
        def _(b=b):
            left_here(xn.at[col, b], t_zr.at[b])

        @pl.when((b >= z) & (z > 0))
        def _(b=b):
            left_here(xn.at[col, b], t_zl.at[b])

    @pl.when(z > 0)
    def _():
        pl.semaphore_signal(credit.at[0], inc=1, device_id=at_z(z - 1), device_id_type=MESH)

    @pl.when(z < zs - 1)
    def _():
        pl.semaphore_signal(credit.at[1], inc=1, device_id=at_z(z + 1), device_id_type=MESH)

    h_over(0)
    w_took(2)
    w_took(3)
    h_over(1)
    w_took(1)

    def w_over(p):
        arrived(wo_at(y, p), w_x.at[p])
        copy(wo_at(y, p), wo_at(y, p), w_ys.at[p], w_y.at[p], at_y).start()

    w_over(ccol)
    w_over(xcol)
    w_over(dcol)
    pl.when(z < zs - 1)(lambda: pl.semaphore_wait(credit.at[0], 1))
    pl.when(z > 0)(lambda: pl.semaphore_wait(credit.at[1], 1))
    h_over(2)
    h_over(3)
    for p in range(zs):
        arrived(wo_at(1 - y, p), w_y.at[p])

    wide = 2 * LANES
    half = outw // wide
    for j in range(zs):
        b = blocks[j]
        for k in (ccol, dcol):
            arrived(hid_at(b, k), h_r.at[k, b])
        from_left = (b >= z) & (z > 0)
        from_right = (b <= z) & (z < zs - 1)

        @pl.when(from_left)
        def _(b=b):
            arrived(xn.at[0, b], o_r.at[0, b])

        @pl.when(from_right)
        def _(b=b):
            slot = jnp.where(b == z, 2, 0)
            arrived(xn.at[slot, b], o_r.at[1, b])

        @pl.loop(0, 2 * half)
        def _(n, b=b, j=j, from_left=from_left, from_right=from_right):
            yy, at = n // half, n % half
            value = dot(hid[b], wo[yy, :, pl.ds(pl.multiple_of(at * wide, wide), wide)])
            lanes = pl.ds(pl.multiple_of(n * wide, wide), wide)
            if j < zs - 1:
                carried = xn[0, b, :, lanes].astype(F32)
                value = value + jnp.where(from_left | from_right, carried, 0.0)
                xn[1, b, :, lanes] = value.astype(BF16)
            else:
                value = value + jnp.where(from_left, xn[0, b, :, lanes].astype(F32), 0.0)
                value = value + jnp.where(from_right, xn[2, b, :, lanes].astype(F32), 0.0)
                out[:, lanes] = value.astype(BF16)

        if j < zs - 1:

            @pl.when(b > z)
            def _(b=b, j=j):
                copy(xn.at[1, b], xn.at[0, b], o_s.at[j], o_r.at[0, b], at_z(z + 1)).start()

            @pl.when(b < z)
            def _(b=b, j=j):
                slot = jnp.where(b == z - 1, 2, 0)
                copy(xn.at[1, b], xn.at[slot, b], o_s.at[j], o_r.at[1, b], at_z(z - 1)).start()

    for n in range(3):
        left_here(ss.at[col], ss_s.at[n])
    for m in range(zs):
        for i in range(2):
            if m:
                left_here(gl_at(z, y, i), g_zs.at[m, i])
            left_here(gl_at(near[m], y, i), g_ys.at[m, i])
        if m:
            left_here(wo_at(w_slab, w_block), w_zs.at[m])
        pl.when(near[m] != col)(lambda m=m: left_here(wo_at(y, col), w_xs.at[m]))
        left_here(wo_at(y, m), w_ys.at[m])
    for j in range(zs):
        left_here(hid_at(blocks[j], col), h_x.at[j])
        left_here(hid_at(blocks[j], col), h_c.at[j])
        left_here(hid_at(blocks[j], xcol), h_d.at[j])
        if j < zs - 1:
            left_here(xn.at[1, blocks[j]], o_s.at[j])


def scratch_of(zs, size, width, depth, part, outw):
    cols = zs
    dma = pltpu.SemaphoreType.DMA
    buffers = [
        ((cols, zs, size, width), BF16),
        ((zs, 2, depth, 2 * part), BF16),
        ((zs, size, 2 * part), F32),
        ((zs, size, cols * part), BF16),
        ((3, cols * part, outw), BF16),
        ((cols, size, LANES), F32),
    ]
    sems = [
        (4,), (3,), (cols,), (cols, zs), (zs,), (zs,), (zs,), (zs,), (zs,), (zs, 2), (zs, 2), (zs, 2), (zs, 2),
        (zs,), (zs,), (cols,), (zs,), (cols,), (cols,), (cols, zs), (zs,), (zs,), (zs,), (2, zs), (zs,),
    ]
    return buffers, [dma(s) for s in sems] + [pltpu.SemaphoreType.REGULAR((2,))]


def fused(zs, buffers, sems, tokens, norm_gain, gate_weight, linear_weight, output_weight):
    anywhere = pl.BlockSpec(memory_space=pl.ANY)
    vmem = pl.BlockSpec(memory_space=pltpu.VMEM)
    return pl.pallas_call(
        functools.partial(body, zs),
        out_shape=jax.ShapeDtypeStruct(tokens.shape, BF16),
        in_specs=[anywhere, vmem, anywhere, anywhere, anywhere],
        out_specs=vmem,
        scratch_shapes=[pltpu.VMEM(shape, kind) for shape, kind in buffers] + sems,
        compiler_params=pltpu.CompilerParams(
            collective_id=0, has_side_effects=True, vmem_limit_bytes=VMEM_LIMIT
        ),
        name="ffn",
    )(tokens, norm_gain.reshape(1, -1), gate_weight, linear_weight, output_weight)


def solution(mesh):
    rows, cols = mesh.shape["row"], mesh.shape["col"]
    zs, xs = rows // 2, cols // 2

    def local(tokens, norm_gain, gate_weight, linear_weight, output_weight):
        args = (tokens, norm_gain, gate_weight, linear_weight, output_weight)
        size, width = tokens.shape
        depth, units = gate_weight.shape
        outw = output_weight.shape[1]
        part = units // zs
        fits = xs == 2 and zs == cols == 4 and units % (zs * LANES) == 0
        fits = fits and 2 * depth == width and 2 * outw == width and outw % (2 * LANES) == 0
        fits = fits and size % 64 == 0
        if fits:
            buffers, sems = scratch_of(zs, size, width, depth, part, outw)
            held = sum(functools.reduce(lambda a, b: a * b, s) * jnp.dtype(k).itemsize for s, k in buffers)
            if held <= SCRATCH_MOST:
                return fused(zs, buffers, sems, *args)
        return gathered(*args)

    return jax.shard_map(
        local,
        mesh=mesh,
        in_specs=(P("row", "col"), P("col"), P("row", "col"), P("row", "col"), P("col", "row")),
        out_specs=P("row", "col"),
        check_vma=False,
    )
```

```python
import functools

import jax
import jax.numpy as jnp
from jax import lax
from jax.experimental import pallas as pl
from jax.experimental.pallas import tpu as pltpu
from jax.sharding import PartitionSpec as P

LANES = 128
VMEM_LIMIT = 67043328
SCRATCH_MOST = 61 << 20
MESH = pl.DeviceIdType.MESH
F32 = jnp.float32
BF16 = jnp.bfloat16


def gathered(tokens, norm_gain, gate_weight, linear_weight, output_weight):
    whole = lax.all_gather(tokens, "col", axis=1, tiled=True)
    gain_all = lax.all_gather(norm_gain, "col", axis=0, tiled=True)
    normed = rms_normed(whole, gain_all)
    gate = dot(normed, lax.all_gather(gate_weight, "row", axis=0, tiled=True))
    linear = dot(normed, lax.all_gather(linear_weight, "row", axis=0, tiled=True))
    hidden = (jax.nn.gelu(gate, approximate=True) * linear).astype(BF16)
    terms = dot(hidden, lax.all_gather(output_weight, "row", axis=1, tiled=True))
    return lax.psum_scatter(terms, "col", scatter_dimension=1, tiled=True).astype(BF16)


def dot(left, right):
    return jnp.dot(left, right, preferred_element_type=F32)


def rms_normed(whole, gain_all):
    values = whole.astype(F32)
    meansq = jnp.mean(values * values, axis=-1, keepdims=True)
    return (values * lax.rsqrt(meansq + 1e-06) * gain_all.astype(F32)).astype(BF16)


def pick(index, table):
    value = jnp.int32(table[0])
    for at in range(1, len(table)):
        value = jnp.where(index == at, jnp.int32(table[at]), value)
    return value


def body(zs, tokens, gain, gate_w, linear_w, out_w, out, xn, gl, acc, hid, wo, ss, *sems):
    (loc, ss_s, ss_r, t_r, t_zr, t_zl, t_x, t_c, t_d, g_z, g_y, g_zs, g_ys, w_z, w_zs, w_x, w_xs,
     w_y, w_ys, h_r, h_x, h_c, h_d, o_r, o_s, credit) = sems
    size, width = tokens.shape
    part = hid.shape[2] // zs
    outw = out_w.shape[1]
    features = width * zs
    wide = outw // 2
    row, col = lax.axis_index("row"), lax.axis_index("col")
    z, y = row // 2, row % 2
    x, core = col // 2, col % 2
    xcol = (1 - x) * 2 + core
    ccol = x * 2 + 1 - core
    dcol = (1 - x) * 2 + 1 - core
    near = [z, z + 1 - 2 * (z % 2), zs - 1 - z, (z + 2) % zs]
    inner = (z > 0) & (z < zs - 1)
    outer = jnp.logical_not(inner)
    at_x, at_c, at_d = (row, xcol), (row, ccol), (row, dcol)
    at_y = (z * 2 + 1 - y, col)

    def at_z(to):
        return (to * 2 + y, col)

    def copy(src, dst, send, recv, to):
        return pltpu.make_async_remote_copy(
            src_ref=src, dst_ref=dst, send_sem=send, recv_sem=recv, device_id=to, device_id_type=MESH
        )

    def arrived(ref, sem):
        copy(ref, ref, sem, sem, at_c).wait_recv()

    def left_here(ref, sem):
        copy(ref, ref, sem, sem, at_c).wait_send()

    def gl_at(zz, yy, i):
        return gl.at[zz, yy, :, pl.ds(i * part, part)]

    def wo_at(slab, block, h):
        rows = pl.ds(pl.multiple_of(block * part, 128), part)
        return wo.at[slab, rows, pl.ds(h * wide, wide)]

    def out_rows(to, h):
        return out_w.at[pl.ds(pl.multiple_of(to * part, 128), part), pl.ds(h * wide, wide)]

    def hid_at(b, k):
        return hid.at[b, :, pl.ds(pl.multiple_of(k * part, 128), part)]

    def cols_of(w, to):
        return w.at[:, pl.ds(pl.multiple_of(to * part, 128), part)]

    own = xn.at[col, z]
    w_slab, w_block = jnp.where(z == col, y, 2), jnp.where(z == col, col, z)
    ins = [
        pltpu.make_async_copy(tokens, own, loc.at[0]),
        pltpu.make_async_copy(cols_of(gate_w, z), gl_at(z, y, 0), loc.at[1]),
        pltpu.make_async_copy(cols_of(linear_w, z), gl_at(z, y, 1), loc.at[2]),
        pltpu.make_async_copy(out_rows(z, 0), wo_at(w_slab, w_block, 0), loc.at[3]),
        pltpu.make_async_copy(out_rows(z, 1), wo_at(w_slab, w_block, 1), loc.at[4]),
    ]
    for each in ins:
        each.start()

    barrier = pltpu.get_barrier_semaphore()
    peers = [at_z(near[1]), at_z(near[2]), at_z(near[3]), at_y, at_x, at_c, at_d]
    for peer in peers:
        pl.semaphore_signal(barrier, inc=1, device_id=peer, device_id_type=MESH)

    ins[0].wait()
    piece = 64

    @pl.loop(0, size // piece)
    def _(i):
        rows = pl.ds(pl.multiple_of(i * piece, piece), piece)
        values = xn[col, z, rows, :].astype(F32)
        sums = jnp.sum(values * values, axis=-1, keepdims=True)
        ss[col, rows, :] = jnp.broadcast_to(sums, (piece, LANES))

    pl.semaphore_wait(barrier, len(peers))

    def g_send(m, i):
        to = near[m]
        copy(
            cols_of((gate_w, linear_w)[i], to), gl_at(z, y, i), g_zs.at[m, i], g_z.at[z, i], at_z(to)
        ).start()

    def g_pass(zz, i):
        ref = gl_at(zz, y, i)
        copy(ref, ref, g_ys.at[zz, i], g_y.at[zz, i], at_y).start()

    def g_took(zz, i):
        arrived(gl_at(zz, y, i), g_z.at[zz, i])
        g_pass(zz, i)

    g_send(1, 0)
    pl.when(inner)(lambda: g_send(2, 0))
    for n, peer in enumerate((at_x, at_c, at_d)):
        copy(ss.at[col], ss.at[col], ss_s.at[n], ss_r.at[col], peer).start()
    ins[1].wait()
    g_pass(z, 0)
    ins[2].wait()
    g_pass(z, 1)
    for k in (xcol, ccol, dcol):
        arrived(ss.at[k], ss_r.at[k])

    @pl.loop(0, size // piece)
    def _(i):
        rows = pl.ds(pl.multiple_of(i * piece, piece), piece)
        total = ss[0, rows, :]
        for k in range(1, zs):
            total = total + ss[k, rows, :]
        scale = lax.rsqrt(total * (1.0 / features) + 1e-06)
        scale = jnp.concatenate([scale] * (width // LANES), axis=1)
        values = xn[col, z, rows, :].astype(F32) * scale * gain[...].astype(F32)
        xn[col, z, rows, :] = values.astype(BF16)

    def t_right(b):
        copy(xn.at[col, b], xn.at[col, b], t_zr.at[b], t_r.at[col, b], at_z(z + 1)).start()

    def t_left(b):
        copy(xn.at[col, b], xn.at[col, b], t_zl.at[b], t_r.at[col, b], at_z(z - 1)).start()

    def t_col(b):
        copy(xn.at[col, b], xn.at[col, b], t_x.at[b], t_r.at[col, b], at_x).start()
        copy(xn.at[col, b], xn.at[col, b], t_c.at[b], t_r.at[col, b], at_c).start()

    def t_over(b):
        arrived(xn.at[xcol, b], t_r.at[xcol, b])
        copy(xn.at[xcol, b], xn.at[xcol, b], t_d.at[b], t_r.at[xcol, b], at_c).start()

    def w_place(zz):
        return jnp.where(zz == col, y, 2), jnp.where(zz == col, col, zz)

    def w_out(m, h):
        zz = near[m]
        ref = wo_at(*w_place(zz), h)

        @pl.when(zz == col)
        def _():
            copy(ref, ref, w_ys.at[col, h], w_y.at[col, h], at_y).start()

        @pl.when(zz != col)
        def _():
            copy(ref, wo_at(y, col, h), w_xs.at[m, h], w_x.at[col, h], (row, zz)).start()

    def w_send(m, h):
        to = near[m]
        copy(out_rows(to, h), wo_at(w_slab, w_block, h), w_zs.at[m, h], w_z.at[z, h], at_z(to)).start()

    def w_took(m, h):
        arrived(wo_at(*w_place(near[m]), h), w_z.at[near[m], h])
        w_out(m, h)

    def w_over(p, h):
        arrived(wo_at(y, p, h), w_x.at[p, h])
        copy(wo_at(y, p, h), wo_at(y, p, h), w_ys.at[p, h], w_y.at[p, h], at_y).start()

    def t_step(s):
        @pl.when(z >= s)
        def _():
            b = z - s
            arrived(xn.at[col, b], t_r.at[col, b])
            pl.when(z < zs - 1)(lambda: t_right(b))
            t_col(b)

        @pl.when(z + s < zs)
        def _():
            b = z + s
            arrived(xn.at[col, b], t_r.at[col, b])
            pl.when(z > 0)(lambda: t_left(b))
            t_col(b)

    def t_over_step(s):
        pl.when(z >= s)(lambda: t_over(z - s))
        pl.when(z + s < zs)(lambda: t_over(z + s))

    far_inner, far_outer = ((2, 1), (3, 0), (3, 1)), ((3, 0), (3, 1), (2, 0), (2, 1))

    def both(on_inner, on_outer):
        pl.when(inner)(on_inner)
        pl.when(outer)(on_outer)

    def stage(k):
        def on(pieces):
            if 0 < k <= len(pieces):
                left_here(gl_at(z, y, 0), g_zs.at[pieces[k - 1]])
            if k < len(pieces):
                g_send(*pieces[k])

        both(lambda: on(far_inner), lambda: on(far_outer))

    def w_stage(h):
        if h:
            for m in (2, 3):
                left_here(wo_at(w_slab, w_block, 0), w_zs.at[m, 0])

        def on(order):
            for m in order:
                w_send(m, h)

        both(lambda: on((2, 3)), lambda: on((3, 2)))

    pl.when(z < zs - 1)(lambda: t_right(z))
    pl.when(z > 0)(lambda: t_left(z))
    t_col(z)
    pl.when(outer)(lambda: g_send(1, 1))
    third = jnp.where(inner, near[2], near[3])
    last = jnp.where(inner, near[3], near[2])
    g_took(near[1], 0)
    pl.when(inner)(lambda: g_took(third, 0))
    t_step(1)

    pl.when(inner)(lambda: g_took(near[1], 1))
    t_step(2)
    stage(0)
    pl.when(inner)(lambda: g_send(1, 1))
    t_step(3)
    t_over(z)
    t_over_step(1)
    stage(1)
    for h in range(2):
        w_send(1, h)

    def on_inner():
        g_took(third, 1)
        g_took(last, 0)

    both(on_inner, lambda: g_took(near[1], 1))
    t_over_step(2)
    t_over_step(3)
    for h in range(2):
        ins[3 + h].wait()
        w_out(0, h)

    tile = 2 * LANES
    tiles = 2 * part // tile
    depth = gl.shape[2]

    def product(kk, b, n, yys):
        lanes = pl.ds(pl.multiple_of(n * tile, tile), tile)
        value = None
        for yy in yys:
            columns = pl.ds(pl.multiple_of(yy * depth, depth), depth)
            term = dot(xn[kk, b, :, columns], gl[kk, yy, :, lanes])
            value = term if value is None else value + term
        return value, lanes

    def inputs(kk, first, yys):
        @pl.loop(0, zs * tiles)
        def _(i):
            b, n = i // tiles, i % tiles
            value, lanes = product(kk, b, n, yys)
            if first:
                acc[b, :, lanes] = value
            else:
                acc[b, :, lanes] = acc[b, :, lanes] + value

    def gl_whole(zz):
        for i in range(2):
            arrived(gl_at(zz, 1 - y, i), g_y.at[zz, i])

    for b in range(zs):
        for k in (ccol, dcol):
            arrived(xn.at[k, b], t_r.at[k, b])
    gl_whole(z)
    inputs(z, True, (0, 1))
    stage(2)
    both(lambda: g_took(last, 1), lambda: g_took(third, 0))
    gl_whole(near[1])
    inputs(near[1], False, (0, 1))
    stage(3)

    def on_outer():
        g_took(third, 1)
        g_took(last, 0)

    pl.when(outer)(on_outer)
    gl_whole(third)
    inputs(third, False, (0, 1))
    stage(4)
    w_stage(0)
    pl.when(outer)(lambda: g_took(last, 1))
    inputs(last, False, (y,))

    orders = [sorted(range(zs), key=lambda b, at=at: -abs(b - at)) for at in range(zs)]
    blocks = [pick(z, [order[j] for order in orders]) for j in range(zs)]

    gl_whole(last)
    cut = 64

    def h_send(j):
        b = blocks[j]
        copy(hid_at(b, col), hid_at(b, col), h_x.at[j], h_r.at[col, b], at_x).start()
        copy(hid_at(b, col), hid_at(b, col), h_c.at[j], h_r.at[col, b], at_c).start()

    for j in range(zs):
        b = blocks[j]

        @pl.loop(0, tiles)
        def _(n, b=b):
            value, lanes = product(last, b, n, (1 - y,))
            acc[b, :, lanes] = acc[b, :, lanes] + value

        @pl.loop(0, size // cut)
        def _(i, b=b):
            rows = pl.ds(pl.multiple_of(i * cut, cut), cut)
            gate = acc[b, rows, :part]
            linear = acc[b, rows, part:]
            value = (jax.nn.gelu(gate, approximate=True) * linear).astype(BF16)
            hid[b, rows, pl.ds(pl.multiple_of(col * part, 128), part)] = value

        if j < 2:
            h_send(j)

    def h_over(j):
        b = blocks[j]
        arrived(hid_at(b, xcol), h_r.at[xcol, b])
        copy(hid_at(b, xcol), hid_at(b, xcol), h_d.at[j], h_r.at[xcol, b], at_c).start()

    for b in range(zs):
        left_here(xn.at[col, b], t_x.at[b])
        left_here(xn.at[col, b], t_c.at[b])
        left_here(xn.at[xcol, b], t_d.at[b])

        @pl.when((b <= z) & (z < zs - 1))
        def _(b=b):
            left_here(xn.at[col, b], t_zr.at[b])

        @pl.when((b >= z) & (z > 0))
        def _(b=b):
            left_here(xn.at[col, b], t_zl.at[b])

    @pl.when(z > 0)
    def _():
        pl.semaphore_signal(credit.at[0], inc=1, device_id=at_z(z - 1), device_id_type=MESH)

    @pl.when(z < zs - 1)
    def _():
        pl.semaphore_signal(credit.at[1], inc=1, device_id=at_z(z + 1), device_id_type=MESH)

    def outputs(h, j):
        b = blocks[j]

        @pl.loop(0, 2)
        def _(yy):
            value = dot(hid[b], wo[yy, :, pl.ds(h * wide, wide)])
            acc[b, :, pl.ds(pl.multiple_of(h * outw + yy * wide, wide), wide)] = value

    def half_of(slot, b, h):
        return xn.at[slot, b, :, pl.ds(h * outw, outw)]

    def carries(h, b):
        from_left = (b >= z) & (z > 0)
        from_right = (b <= z) & (z < zs - 1)
        slot = jnp.where(b == z, 2, 0)
        pl.when(from_left)(lambda: arrived(half_of(0, b, h), o_r.at[0, b, h]))
        pl.when(from_right)(lambda: arrived(half_of(slot, b, h), o_r.at[1, b, h]))
        return from_left, from_right

    def relay(h, j):
        b = blocks[j]
        from_left, from_right = carries(h, b)
        lanes = pl.ds(h * outw, outw)
        carry = from_left | from_right

        @pl.loop(0, size // cut)
        def _(i):
            rows = pl.ds(pl.multiple_of(i * cut, cut), cut)
            value = acc[b, rows, lanes] + jnp.where(carry, xn[0, b, rows, lanes].astype(F32), 0.0)
            xn[1, b, rows, lanes] = value.astype(BF16)

        @pl.when(b > z)
        def _():
            copy(half_of(1, b, h), half_of(0, b, h), o_s.at[j, h], o_r.at[0, b, h], at_z(z + 1)).start()

        @pl.when(b < z)
        def _():
            slot = jnp.where(b == z - 1, 2, 0)
            copy(half_of(1, b, h), half_of(slot, b, h), o_s.at[j, h], o_r.at[1, b, h], at_z(z - 1)).start()

    def finish(h):
        from_left, from_right = carries(h, z)

        @pl.loop(0, size // cut)
        def _(i):
            rows = pl.ds(pl.multiple_of(i * cut, cut), cut)
            for yy in range(2):
                lanes = pl.ds(h * outw + yy * wide, wide)
                value = acc[z, rows, lanes]
                value = value + jnp.where(from_left, xn[0, z, rows, lanes].astype(F32), 0.0)
                value = value + jnp.where(from_right, xn[2, z, rows, lanes].astype(F32), 0.0)
                out[rows, pl.ds(yy * outw + h * wide, wide)] = value.astype(BF16)

    def hid_whole(j):
        for k in (ccol, dcol):
            arrived(hid_at(blocks[j], k), h_r.at[k, blocks[j]])

    def wo_whole(h):
        for p in range(zs):
            arrived(wo_at(1 - y, p, h), w_y.at[p, h])

    w_stage(1)
    for m in range(1, zs):
        w_took(m, 0)
    h_send(2)
    h_over(0)
    for p in (ccol, xcol, dcol):
        w_over(p, 0)
    h_over(1)
    wo_whole(0)
    hid_whole(0)
    outputs(0, 0)
    pl.when(z < zs - 1)(lambda: pl.semaphore_wait(credit.at[0], 1))
    pl.when(z > 0)(lambda: pl.semaphore_wait(credit.at[1], 1))
    relay(0, 0)
    hid_whole(1)
    outputs(0, 1)
    relay(0, 1)
    for m in range(1, zs):
        w_took(m, 1)
    h_send(3)
    h_over(2)
    for p in (ccol, xcol, dcol):
        w_over(p, 1)
    hid_whole(2)
    outputs(0, 2)
    relay(0, 2)
    wo_whole(1)
    for j in range(zs - 1):
        outputs(1, j)
        relay(1, j)
    h_over(3)
    hid_whole(3)
    for h in range(2):
        outputs(h, zs - 1)
    for h in range(2):
        finish(h)

    for n in range(3):
        left_here(ss.at[col], ss_s.at[n])
    pl.when(inner)(lambda: left_here(gl_at(z, y, 0), g_zs.at[2, 0]))
    for m in range(zs):
        for i in range(2):
            if m == 1:
                left_here(gl_at(z, y, i), g_zs.at[m, i])
            left_here(gl_at(m, y, i), g_ys.at[m, i])
        for h in range(2):
            if m == 1 or m and h:
                left_here(wo_at(w_slab, w_block, h), w_zs.at[m, h])
            pl.when(near[m] != col)(lambda m=m, h=h: left_here(wo_at(y, col, h), w_xs.at[m, h]))
            left_here(wo_at(y, m, h), w_ys.at[m, h])
    for j in range(zs):
        left_here(hid_at(blocks[j], col), h_x.at[j])
        left_here(hid_at(blocks[j], col), h_c.at[j])
        left_here(hid_at(blocks[j], xcol), h_d.at[j])
        if j < zs - 1:
            for h in range(2):
                left_here(half_of(1, blocks[j], h), o_s.at[j, h])


def scratch_of(zs, size, width, depth, part, outw):
    cols = zs
    dma = pltpu.SemaphoreType.DMA
    buffers = [
        ((cols, zs, size, width), BF16),
        ((zs, 2, depth, 2 * part), BF16),
        ((zs, size, 2 * part), F32),
        ((zs, size, cols * part), BF16),
        ((3, cols * part, outw), BF16),
        ((cols, size, LANES), F32),
    ]
    sems = [
        (5,), (3,), (cols,), (cols, zs), (zs,), (zs,), (zs,), (zs,), (zs,), (zs, 2), (zs, 2), (zs, 2), (zs, 2),
        (zs, 2), (zs, 2), (cols, 2), (zs, 2), (cols, 2), (cols, 2), (cols, zs), (zs,), (zs,), (zs,), (2, zs, 2), (zs, 2),
    ]
    return buffers, [dma(s) for s in sems] + [pltpu.SemaphoreType.REGULAR((2,))]


def fused(zs, buffers, sems, tokens, norm_gain, gate_weight, linear_weight, output_weight):
    anywhere = pl.BlockSpec(memory_space=pl.ANY)
    vmem = pl.BlockSpec(memory_space=pltpu.VMEM)
    return pl.pallas_call(
        functools.partial(body, zs),
        out_shape=jax.ShapeDtypeStruct(tokens.shape, BF16),
        in_specs=[anywhere, vmem, anywhere, anywhere, anywhere],
        out_specs=vmem,
        scratch_shapes=[pltpu.VMEM(shape, kind) for shape, kind in buffers] + sems,
        compiler_params=pltpu.CompilerParams(
            collective_id=0, has_side_effects=True, vmem_limit_bytes=VMEM_LIMIT
        ),
        name="ffn",
    )(tokens, norm_gain.reshape(1, -1), gate_weight, linear_weight, output_weight)


def solution(mesh):
    rows, cols = mesh.shape["row"], mesh.shape["col"]
    zs, xs = rows // 2, cols // 2

    def local(tokens, norm_gain, gate_weight, linear_weight, output_weight):
        args = (tokens, norm_gain, gate_weight, linear_weight, output_weight)
        size, width = tokens.shape
        depth, units = gate_weight.shape
        outw = output_weight.shape[1]
        part = units // zs
        fits = xs == 2 and zs == cols == 4 and units % (zs * LANES) == 0
        fits = fits and 2 * depth == width and 2 * outw == width and outw % (2 * LANES) == 0
        fits = fits and size % 64 == 0
        if fits:
            buffers, sems = scratch_of(zs, size, width, depth, part, outw)
            held = sum(functools.reduce(lambda a, b: a * b, s) * jnp.dtype(k).itemsize for s, k in buffers)
            if held <= SCRATCH_MOST:
                return fused(zs, buffers, sems, *args)
        return gathered(*args)

    return jax.shard_map(
        local,
        mesh=mesh,
        in_specs=(P("row", "col"), P("col"), P("row", "col"), P("row", "col"), P("col", "row")),
        out_specs=P("row", "col"),
        check_vma=False,
    )
```

```python
import functools

import jax
import jax.numpy as jnp
from jax import lax
from jax.experimental import pallas as pl
from jax.experimental.pallas import tpu as pltpu
from jax.sharding import PartitionSpec as P

LANES = 128
VMEM_LIMIT = 67043328
SCRATCH_MOST = 61 << 20
MESH = pl.DeviceIdType.MESH
F32 = jnp.float32
BF16 = jnp.bfloat16


def gathered(tokens, norm_gain, gate_weight, linear_weight, output_weight):
    whole = lax.all_gather(tokens, "col", axis=1, tiled=True)
    gain_all = lax.all_gather(norm_gain, "col", axis=0, tiled=True)
    normed = rms_normed(whole, gain_all)
    gate = dot(normed, lax.all_gather(gate_weight, "row", axis=0, tiled=True))
    linear = dot(normed, lax.all_gather(linear_weight, "row", axis=0, tiled=True))
    hidden = (jax.nn.gelu(gate, approximate=True) * linear).astype(BF16)
    terms = dot(hidden, lax.all_gather(output_weight, "row", axis=1, tiled=True))
    return lax.psum_scatter(terms, "col", scatter_dimension=1, tiled=True).astype(BF16)


def dot(left, right):
    return jnp.dot(left, right, preferred_element_type=F32)


def rms_normed(whole, gain_all):
    values = whole.astype(F32)
    meansq = jnp.mean(values * values, axis=-1, keepdims=True)
    return (values * lax.rsqrt(meansq + 1e-06) * gain_all.astype(F32)).astype(BF16)


def pick(index, table):
    value = jnp.int32(table[0])
    for at in range(1, len(table)):
        value = jnp.where(index == at, jnp.int32(table[at]), value)
    return value


def body(zs, tokens, gain, gate_w, linear_w, out_w, out, xn, gl, acc, hid, wo, ss, *sems):
    (loc, ss_s, ss_r, t_r, t_zr, t_zl, t_x, t_c, t_d, g_z, g_y, g_zs, g_ys, w_z, w_zs, w_x, w_xs,
     w_y, w_ys, h_r, h_x, h_c, h_d, o_r, o_s, credit) = sems
    size, width = tokens.shape
    part = hid.shape[2] // zs
    outw = out_w.shape[1]
    features = width * zs
    wide = outw // 2
    first_share = (part // LANES + 1) // 2 * LANES
    shares = (first_share, part - first_share)
    starts = (0, 2 * first_share)
    row, col = lax.axis_index("row"), lax.axis_index("col")
    z, y = row // 2, row % 2
    x, core = col // 2, col % 2
    xcol = (1 - x) * 2 + core
    ccol = x * 2 + 1 - core
    dcol = (1 - x) * 2 + 1 - core
    near = [z, z + 1 - 2 * (z % 2), zs - 1 - z, (z + 2) % zs]
    inner = (z > 0) & (z < zs - 1)
    outer = jnp.logical_not(inner)
    at_x, at_c, at_d = (row, xcol), (row, ccol), (row, dcol)
    at_y = (z * 2 + 1 - y, col)

    def at_z(to):
        return (to * 2 + y, col)

    def copy(src, dst, send, recv, to):
        return pltpu.make_async_remote_copy(
            src_ref=src, dst_ref=dst, send_sem=send, recv_sem=recv, device_id=to, device_id_type=MESH
        )

    def arrived(ref, sem):
        copy(ref, ref, sem, sem, at_c).wait_recv()

    def left_here(ref, sem):
        copy(ref, ref, sem, sem, at_c).wait_send()

    def gl_at(zz, yy, i):
        return gl.at[zz, yy, :, pl.ds(starts[i], 2 * shares[i])]

    def gl_of(zz, yy, i, which):
        return gl.at[zz, yy, :, pl.ds(starts[i] + which * shares[i], shares[i])]

    def wo_at(slab, block, h):
        rows = pl.ds(pl.multiple_of(block * part, 128), part)
        return wo.at[slab, rows, pl.ds(h * wide, wide)]

    def out_rows(to, h):
        return out_w.at[pl.ds(pl.multiple_of(to * part, 128), part), pl.ds(h * wide, wide)]

    def hid_at(b, k, i):
        return hid.at[b, :, pl.ds(pl.multiple_of(k * part + i * first_share, LANES), shares[i])]

    def cols_of(w, to, i):
        return w.at[:, pl.ds(pl.multiple_of(to * part + i * first_share, LANES), shares[i])]

    own = xn.at[col, z]
    w_slab, w_block = jnp.where(z == col, y, 2), jnp.where(z == col, col, z)
    ins = [
        pltpu.make_async_copy(tokens, own, loc.at[0]),
        pltpu.make_async_copy(out_rows(z, 0), wo_at(w_slab, w_block, 0), loc.at[1]),
        pltpu.make_async_copy(out_rows(z, 1), wo_at(w_slab, w_block, 1), loc.at[2]),
    ]
    ins += [
        pltpu.make_async_copy(cols_of(w, z, i), gl_of(z, y, i, which), loc.at[3 + 2 * i + which])
        for i in range(2)
        for which, w in enumerate((gate_w, linear_w))
    ]
    for each in ins:
        each.start()

    barrier = pltpu.get_barrier_semaphore()
    peers = [at_z(near[1]), at_z(near[2]), at_z(near[3]), at_y, at_x, at_c, at_d]
    for peer in peers:
        pl.semaphore_signal(barrier, inc=1, device_id=peer, device_id_type=MESH)

    ins[0].wait()
    piece = 64

    @pl.loop(0, size // piece)
    def _(i):
        rows = pl.ds(pl.multiple_of(i * piece, piece), piece)
        values = xn[col, z, rows, :].astype(F32)
        sums = jnp.sum(values * values, axis=-1, keepdims=True)
        ss[col, rows, :] = jnp.broadcast_to(sums, (piece, LANES))

    pl.semaphore_wait(barrier, len(peers))

    def g_send(m, i):
        to = near[m]
        for which, w in enumerate((gate_w, linear_w)):
            copy(
                cols_of(w, to, i), gl_of(z, y, i, which), g_zs.at[m, i], g_z.at[z, i], at_z(to)
            ).start()

    def g_pass(zz, i):
        ref = gl_at(zz, y, i)
        copy(ref, ref, g_ys.at[zz, i], g_y.at[zz, i], at_y).start()

    def g_took(zz, i):
        arrived(gl_at(zz, y, i), g_z.at[zz, i])
        g_pass(zz, i)

    g_send(1, 0)
    pl.when(inner)(lambda: g_send(2, 0))
    for n, peer in enumerate((at_x, at_c, at_d)):
        copy(ss.at[col], ss.at[col], ss_s.at[n], ss_r.at[col], peer).start()
    for i in range(2):
        for which in range(2):
            ins[3 + 2 * i + which].wait()
        g_pass(z, i)
    for k in (xcol, ccol, dcol):
        arrived(ss.at[k], ss_r.at[k])

    @pl.loop(0, size // piece)
    def _(i):
        rows = pl.ds(pl.multiple_of(i * piece, piece), piece)
        total = ss[0, rows, :]
        for k in range(1, zs):
            total = total + ss[k, rows, :]
        scale = lax.rsqrt(total * (1.0 / features) + 1e-06)
        scale = jnp.concatenate([scale] * (width // LANES), axis=1)
        values = xn[col, z, rows, :].astype(F32) * scale * gain[...].astype(F32)
        xn[col, z, rows, :] = values.astype(BF16)

    def t_right(b):
        copy(xn.at[col, b], xn.at[col, b], t_zr.at[b], t_r.at[col, b], at_z(z + 1)).start()

    def t_left(b):
        copy(xn.at[col, b], xn.at[col, b], t_zl.at[b], t_r.at[col, b], at_z(z - 1)).start()

    def t_col(b):
        copy(xn.at[col, b], xn.at[col, b], t_x.at[b], t_r.at[col, b], at_x).start()
        copy(xn.at[col, b], xn.at[col, b], t_c.at[b], t_r.at[col, b], at_c).start()

    def t_over(b):
        arrived(xn.at[xcol, b], t_r.at[xcol, b])
        copy(xn.at[xcol, b], xn.at[xcol, b], t_d.at[b], t_r.at[xcol, b], at_c).start()

    def w_place(zz):
        return jnp.where(zz == col, y, 2), jnp.where(zz == col, col, zz)

    def w_out(m, h):
        zz = near[m]
        ref = wo_at(*w_place(zz), h)

        @pl.when(zz == col)
        def _():
            copy(ref, ref, w_ys.at[col, h], w_y.at[col, h], at_y).start()

        @pl.when(zz != col)
        def _():
            copy(ref, wo_at(y, col, h), w_xs.at[m, h], w_x.at[col, h], (row, zz)).start()

    def w_send(m, h):
        to = near[m]
        copy(out_rows(to, h), wo_at(w_slab, w_block, h), w_zs.at[m, h], w_z.at[z, h], at_z(to)).start()

    def w_took(m, h):
        arrived(wo_at(*w_place(near[m]), h), w_z.at[near[m], h])
        w_out(m, h)

    def w_over(p, h):
        arrived(wo_at(y, p, h), w_x.at[p, h])
        copy(wo_at(y, p, h), wo_at(y, p, h), w_ys.at[p, h], w_y.at[p, h], at_y).start()

    def t_step(s):
        below, above = z >= s, z + s < zs

        def from_below():
            arrived(xn.at[col, z - s], t_r.at[col, z - s])
            pl.when(z < zs - 1)(lambda: t_right(z - s))

        def from_above():
            arrived(xn.at[col, z + s], t_r.at[col, z + s])
            pl.when(z > 0)(lambda: t_left(z + s))

        pl.when(below & (z < zs // 2))(from_below)
        pl.when(above)(from_above)
        pl.when(below & (z >= zs // 2))(from_below)
        pl.when(below)(lambda: t_col(z - s))
        pl.when(above)(lambda: t_col(z + s))

    def t_over_step(s):
        pl.when(z >= s)(lambda: t_over(z - s))
        pl.when(z + s < zs)(lambda: t_over(z + s))

    far_outer = ((3, 0), (2, 0), (3, 1), (2, 1))

    def both(on_inner, on_outer):
        pl.when(inner)(on_inner)
        pl.when(outer)(on_outer)

    def stage(k, pieces):
        if 0 < k <= len(pieces):
            m, i = pieces[k - 1]
            left_here(gl_at(z, y, i), g_zs.at[m, i])
        for n in (0, 1) if k == 0 else (k + 1,):
            if n < len(pieces):
                g_send(*pieces[n])

    def near_out():
        for h in range(2):
            w_send(1, h)

    def w_stage(h):
        if h:
            for m in (2, 3):
                left_here(wo_at(w_slab, w_block, 0), w_zs.at[m, 0])

        def on(order):
            for m in order:
                w_send(m, h)

        both(lambda: on((2, 3) if h else (3,)), lambda: on((3, 2)))

    pl.when(z < zs - 1)(lambda: t_right(z))
    pl.when(z > 0)(lambda: t_left(z))
    t_col(z)
    pl.when(outer)(lambda: g_send(1, 1))
    third = jnp.where(inner, near[2], near[3])
    last = jnp.where(inner, near[3], near[2])
    g_took(near[1], 0)
    t_step(1)

    def early():
        g_took(third, 0)
        g_took(near[1], 1)

    pl.when(inner)(early)
    t_step(2)

    def relayed(up, b):
        left_here(xn.at[col, b], (t_zr if up else t_zl).at[b])

    lower, upper = inner & (z < zs // 2), inner & (z >= zs // 2)
    pl.when(lower)(lambda: relayed(True, z - 1))
    pl.when(upper)(lambda: relayed(False, z + 1))
    @pl.when(inner)
    def _():
        g_send(2, 1)
        w_send(2, 0)

    t_step(3)
    pl.when(outer)(lambda: stage(0, far_outer))
    t_over(z)
    t_over_step(1)

    @pl.when(lower)
    def _():
        relayed(False, z + 1)
        relayed(False, z + 2)

    @pl.when(upper)
    def _():
        relayed(True, z - 1)
        relayed(True, z - 2)

    @pl.when(inner)
    def _():
        g_send(1, 1)
        g_send(3, 0)
        g_took(third, 1)

    t_over_step(2)
    t_over_step(3)
    for h in range(2):
        ins[1 + h].wait()
        w_out(0, h)

    tile = 2 * LANES
    tiles = 2 * part // tile
    depth = gl.shape[2]

    def product(kk, b, n, yys):
        lanes = pl.ds(pl.multiple_of(n * tile, tile), tile)
        value = None
        for yy in yys:
            columns = pl.ds(pl.multiple_of(yy * depth, depth), depth)
            term = dot(xn[kk, b, :, columns], gl[kk, yy, :, lanes])
            value = term if value is None else value + term
        return value, lanes

    def inputs(kk, i, first, yys, block=None):
        count = 2 * shares[i] // tile

        @pl.loop(0, count if block is not None else zs * count)
        def _(n):
            b, at = (n // count, n % count) if block is None else (block, n)
            value, lanes = product(kk, b, starts[i] // tile + at, yys)
            if first:
                acc[b, :, lanes] = value
            else:
                acc[b, :, lanes] = acc[b, :, lanes] + value

    def gl_whole(zz, i):
        arrived(gl_at(zz, 1 - y, i), g_y.at[zz, i])

    cut = 64

    def h_send(j, i):
        b = blocks[j]
        copy(hid_at(b, col, i), hid_at(b, col, i), h_x.at[j, i], h_r.at[col, b, i], at_x).start()
        copy(hid_at(b, col, i), hid_at(b, col, i), h_c.at[j, i], h_r.at[col, b, i], at_c).start()

    def h_over(j, i):
        b = blocks[j]
        arrived(hid_at(b, xcol, i), h_r.at[xcol, b, i])
        copy(hid_at(b, xcol, i), hid_at(b, xcol, i), h_d.at[j, i], h_r.at[xcol, b, i], at_c).start()

    def hidden(j, i):
        b = blocks[j]

        @pl.loop(0, size // cut)
        def _(n):
            rows = pl.ds(pl.multiple_of(n * cut, cut), cut)
            gate = acc[b, rows, pl.ds(starts[i], shares[i])]
            linear = acc[b, rows, pl.ds(starts[i] + shares[i], shares[i])]
            value = (jax.nn.gelu(gate, approximate=True) * linear).astype(BF16)
            hid[b, rows, pl.ds(pl.multiple_of(col * part + i * first_share, LANES), shares[i])] = value

    orders = [sorted(range(zs), key=lambda b, at=at: -abs(b - at)) for at in range(zs)]
    blocks = [pick(z, [order[j] for order in orders]) for j in range(zs)]

    for b in range(zs):
        for k in (ccol, dcol):
            arrived(xn.at[k, b], t_r.at[k, b])
    gl_whole(z, 0)
    inputs(z, 0, True, (0, 1))

    @pl.when(inner)
    def _():
        g_send(3, 1)
        g_took(last, 0)

    pl.when(outer)(lambda: stage(1, far_outer))
    near_out()
    gl_whole(near[1], 0)
    inputs(near[1], 0, False, (0, 1))

    @pl.when(outer)
    def _():
        g_took(near[1], 1)
        g_took(third, 0)

    gl_whole(z, 1)
    inputs(z, 1, True, (0, 1))

    @pl.when(outer)
    def _():
        stage(2, far_outer)
        g_took(last, 0)

    gl_whole(near[1], 1)
    inputs(near[1], 1, False, (0, 1))
    gl_whole(third, 0)
    inputs(third, 0, False, (0, 1))
    pl.when(outer)(lambda: g_took(third, 1))
    gl_whole(last, 0)
    for j in range(zs):
        inputs(last, 0, False, (0, 1), blocks[j])
        hidden(j, 0)
        h_send(j, 0)
    pl.when(outer)(lambda: stage(3, far_outer))
    pl.when(inner)(lambda: g_took(last, 1))
    gl_whole(third, 1)
    inputs(third, 1, False, (0, 1))

    def inner_left():
        for m, i in ((2, 1), (3, 0), (3, 1)):
            left_here(gl_at(z, y, i), g_zs.at[m, i])

    both(inner_left, lambda: stage(4, far_outer))
    w_stage(0)
    pl.when(outer)(lambda: g_took(last, 1))
    inputs(last, 1, False, (y,))
    gl_whole(last, 1)
    for j in range(zs):
        inputs(last, 1, False, (1 - y,), blocks[j])
        hidden(j, 1)
        if j < 2:
            h_send(j, 1)

    for b in range(zs):
        left_here(xn.at[col, b], t_x.at[b])
        left_here(xn.at[col, b], t_c.at[b])
        left_here(xn.at[xcol, b], t_d.at[b])

        @pl.when((b <= z) & (z < zs - 1) & (outer | (b == z)))
        def _(b=b):
            left_here(xn.at[col, b], t_zr.at[b])

        @pl.when((b >= z) & (z > 0) & (outer | (b == z)))
        def _(b=b):
            left_here(xn.at[col, b], t_zl.at[b])

    @pl.when(z > 0)
    def _():
        pl.semaphore_signal(credit.at[0], inc=1, device_id=at_z(z - 1), device_id_type=MESH)

    @pl.when(z < zs - 1)
    def _():
        pl.semaphore_signal(credit.at[1], inc=1, device_id=at_z(z + 1), device_id_type=MESH)

    def outputs(h, j):
        b = blocks[j]

        @pl.loop(0, 2)
        def _(yy):
            value = dot(hid[b], wo[yy, :, pl.ds(h * wide, wide)])
            acc[b, :, pl.ds(pl.multiple_of(h * outw + yy * wide, wide), wide)] = value

    def half_of(slot, b, h):
        return xn.at[slot, b, :, pl.ds(h * outw, outw)]

    def carries(h, b):
        from_left = (b >= z) & (z > 0)
        from_right = (b <= z) & (z < zs - 1)
        slot = jnp.where(b == z, 2, 0)
        pl.when(from_left)(lambda: arrived(half_of(0, b, h), o_r.at[0, b, h]))
        pl.when(from_right)(lambda: arrived(half_of(slot, b, h), o_r.at[1, b, h]))
        return from_left, from_right

    def relay(h, j):
        b = blocks[j]
        from_left, from_right = carries(h, b)
        lanes = pl.ds(h * outw, outw)
        carry = from_left | from_right

        @pl.loop(0, size // cut)
        def _(i):
            rows = pl.ds(pl.multiple_of(i * cut, cut), cut)
            value = acc[b, rows, lanes] + jnp.where(carry, xn[0, b, rows, lanes].astype(F32), 0.0)
            xn[1, b, rows, lanes] = value.astype(BF16)

        @pl.when(b > z)
        def _():
            copy(half_of(1, b, h), half_of(0, b, h), o_s.at[j, h], o_r.at[0, b, h], at_z(z + 1)).start()

        @pl.when(b < z)
        def _():
            slot = jnp.where(b == z - 1, 2, 0)
            copy(half_of(1, b, h), half_of(slot, b, h), o_s.at[j, h], o_r.at[1, b, h], at_z(z - 1)).start()

    def finish(h):
        from_left, from_right = carries(h, z)

        @pl.loop(0, size // cut)
        def _(i):
            rows = pl.ds(pl.multiple_of(i * cut, cut), cut)
            for yy in range(2):
                lanes = pl.ds(h * outw + yy * wide, wide)
                value = acc[z, rows, lanes]
                value = value + jnp.where(from_left, xn[0, z, rows, lanes].astype(F32), 0.0)
                value = value + jnp.where(from_right, xn[2, z, rows, lanes].astype(F32), 0.0)
                out[rows, pl.ds(yy * outw + h * wide, wide)] = value.astype(BF16)

    def hid_whole(j):
        for k in (ccol, dcol):
            for i in range(2):
                arrived(hid_at(blocks[j], k, i), h_r.at[k, blocks[j], i])

    def wo_whole(h):
        for p in range(zs):
            arrived(wo_at(1 - y, p, h), w_y.at[p, h])

    for m in range(1, zs):
        w_took(m, 0)
    h_send(2, 1)
    h_send(3, 1)
    w_stage(1)
    for j in range(zs):
        h_over(j, 0)
    h_over(0, 1)
    h_over(1, 1)
    for p in (ccol, xcol, dcol):
        w_over(p, 0)
    wo_whole(0)
    hid_whole(0)
    outputs(0, 0)
    pl.when(z < zs - 1)(lambda: pl.semaphore_wait(credit.at[0], 1))
    pl.when(z > 0)(lambda: pl.semaphore_wait(credit.at[1], 1))
    pl.when(outer)(lambda: relay(0, 0))
    hid_whole(1)
    outputs(0, 1)
    pl.when(outer)(lambda: relay(0, 1))
    for m in range(1, zs):
        w_took(m, 1)
    h_over(2, 1)
    h_over(3, 1)
    hid_whole(2)
    outputs(0, 2)
    both(lambda: relay(0, 0), lambda: relay(0, 2))
    for p in (ccol, xcol, dcol):
        w_over(p, 1)
    pl.when(inner)(lambda: relay(0, 1))
    pl.when(inner)(lambda: relay(0, 2))
    wo_whole(1)
    for j in range(zs - 1):
        outputs(1, j)
        relay(1, j)
    hid_whole(3)
    for h in range(2):
        outputs(h, zs - 1)
    for h in range(2):
        finish(h)

    for n in range(3):
        left_here(ss.at[col], ss_s.at[n])
    pl.when(inner)(lambda: left_here(gl_at(z, y, 0), g_zs.at[2, 0]))
    for m in range(zs):
        for i in range(2):
            if m == 1:
                left_here(gl_at(z, y, i), g_zs.at[m, i])
            left_here(gl_at(m, y, i), g_ys.at[m, i])
        for h in range(2):
            if m == 1 or m and h:
                left_here(wo_at(w_slab, w_block, h), w_zs.at[m, h])
            pl.when(near[m] != col)(lambda m=m, h=h: left_here(wo_at(y, col, h), w_xs.at[m, h]))
            left_here(wo_at(y, m, h), w_ys.at[m, h])
    for j in range(zs):
        for i in range(2):
            for sem in (h_x, h_c, h_d):
                left_here(hid_at(blocks[j], col, i), sem.at[j, i])
        if j < zs - 1:
            for h in range(2):
                left_here(half_of(1, blocks[j], h), o_s.at[j, h])


def scratch_of(zs, size, width, depth, part, outw):
    cols = zs
    dma = pltpu.SemaphoreType.DMA
    buffers = [
        ((cols, zs, size, width), BF16),
        ((zs, 2, depth, 2 * part), BF16),
        ((zs, size, 2 * part), F32),
        ((zs, size, cols * part), BF16),
        ((3, cols * part, outw), BF16),
        ((cols, size, LANES), F32),
    ]
    sems = [
        (7,), (3,), (cols,), (cols, zs), (zs,), (zs,), (zs,), (zs,), (zs,), (zs, 2), (zs, 2), (zs, 2), (zs, 2),
        (zs, 2), (zs, 2), (cols, 2), (zs, 2), (cols, 2), (cols, 2), (cols, zs, 2), (zs, 2), (zs, 2), (zs, 2), (2, zs, 2),
        (zs, 2),
    ]
    return buffers, [dma(s) for s in sems] + [pltpu.SemaphoreType.REGULAR((2,))]


def fused(zs, buffers, sems, tokens, norm_gain, gate_weight, linear_weight, output_weight):
    anywhere = pl.BlockSpec(memory_space=pl.ANY)
    vmem = pl.BlockSpec(memory_space=pltpu.VMEM)
    return pl.pallas_call(
        functools.partial(body, zs),
        out_shape=jax.ShapeDtypeStruct(tokens.shape, BF16),
        in_specs=[anywhere, vmem, anywhere, anywhere, anywhere],
        out_specs=vmem,
        scratch_shapes=[pltpu.VMEM(shape, kind) for shape, kind in buffers] + sems,
        compiler_params=pltpu.CompilerParams(
            collective_id=0, has_side_effects=True, vmem_limit_bytes=VMEM_LIMIT
        ),
        name="ffn",
    )(tokens, norm_gain.reshape(1, -1), gate_weight, linear_weight, output_weight)


def solution(mesh):
    rows, cols = mesh.shape["row"], mesh.shape["col"]
    zs, xs = rows // 2, cols // 2

    def local(tokens, norm_gain, gate_weight, linear_weight, output_weight):
        args = (tokens, norm_gain, gate_weight, linear_weight, output_weight)
        size, width = tokens.shape
        depth, units = gate_weight.shape
        outw = output_weight.shape[1]
        part = units // zs
        fits = xs == 2 and zs == cols == 4 and units % (zs * LANES) == 0
        fits = fits and 2 * depth == width and 2 * outw == width and outw % (2 * LANES) == 0
        fits = fits and size % 64 == 0
        if fits:
            buffers, sems = scratch_of(zs, size, width, depth, part, outw)
            held = sum(functools.reduce(lambda a, b: a * b, s) * jnp.dtype(k).itemsize for s, k in buffers)
            if held <= SCRATCH_MOST:
                return fused(zs, buffers, sems, *args)
        return gathered(*args)

    return jax.shard_map(
        local,
        mesh=mesh,
        in_specs=(P("row", "col"), P("col"), P("row", "col"), P("row", "col"), P("col", "row")),
        out_specs=P("row", "col"),
        check_vma=False,
    )
```

```python
import functools

import jax
import jax.numpy as jnp
from jax import lax
from jax.experimental import pallas as pl
from jax.experimental.pallas import tpu as pltpu
from jax.sharding import PartitionSpec as P

LANES = 128
VMEM_LIMIT = 67043328
SCRATCH_MOST = 61 << 20
MESH = pl.DeviceIdType.MESH
F32 = jnp.float32
BF16 = jnp.bfloat16


def gathered(tokens, norm_gain, gate_weight, linear_weight, output_weight):
    whole = lax.all_gather(tokens, "col", axis=1, tiled=True)
    gain_all = lax.all_gather(norm_gain, "col", axis=0, tiled=True)
    normed = rms_normed(whole, gain_all)
    gate = dot(normed, lax.all_gather(gate_weight, "row", axis=0, tiled=True))
    linear = dot(normed, lax.all_gather(linear_weight, "row", axis=0, tiled=True))
    hidden = (jax.nn.gelu(gate, approximate=True) * linear).astype(BF16)
    terms = dot(hidden, lax.all_gather(output_weight, "row", axis=1, tiled=True))
    return lax.psum_scatter(terms, "col", scatter_dimension=1, tiled=True).astype(BF16)


def dot(left, right):
    return jnp.dot(left, right, preferred_element_type=F32)


def rms_normed(whole, gain_all):
    values = whole.astype(F32)
    meansq = jnp.mean(values * values, axis=-1, keepdims=True)
    return (values * lax.rsqrt(meansq + 1e-06) * gain_all.astype(F32)).astype(BF16)


def pick(index, table):
    value = jnp.int32(table[0])
    for at in range(1, len(table)):
        value = jnp.where(index == at, jnp.int32(table[at]), value)
    return value


def body(zs, tokens, gain, gate_w, linear_w, out_w, out, xn, gl, acc, hid, wo, ss, *sems):
    (loc, ss_s, ss_r, t_r, t_zr, t_zl, t_x, t_c, t_d, g_z, g_y, g_zs, g_ys, w_z, w_zs, w_x, w_xs,
     w_y, w_ys, h_r, h_x, h_c, h_d, o_r, o_s, credit) = sems
    size, width = tokens.shape
    part = hid.shape[2] // zs
    outw = out_w.shape[1]
    features = width * zs
    wide = outw // 2
    first_share = (part // LANES + 1) // 2 * LANES
    shares = (first_share, part - first_share)
    starts = (0, 2 * first_share)
    row, col = lax.axis_index("row"), lax.axis_index("col")
    z, y = row // 2, row % 2
    x, core = col // 2, col % 2
    xcol = (1 - x) * 2 + core
    ccol = x * 2 + 1 - core
    dcol = (1 - x) * 2 + 1 - core
    near = [z, z + 1 - 2 * (z % 2), zs - 1 - z, (z + 2) % zs]
    inner = (z > 0) & (z < zs - 1)
    outer = jnp.logical_not(inner)
    at_x, at_c, at_d = (row, xcol), (row, ccol), (row, dcol)
    at_y = (z * 2 + 1 - y, col)

    def at_z(to):
        return (to * 2 + y, col)

    def copy(src, dst, send, recv, to):
        return pltpu.make_async_remote_copy(
            src_ref=src, dst_ref=dst, send_sem=send, recv_sem=recv, device_id=to, device_id_type=MESH
        )

    def arrived(ref, sem):
        copy(ref, ref, sem, sem, at_c).wait_recv()

    def left_here(ref, sem):
        copy(ref, ref, sem, sem, at_c).wait_send()

    def gl_at(zz, yy, i):
        return gl.at[zz, yy, :, pl.ds(starts[i], 2 * shares[i])]

    def gl_of(zz, yy, i, which):
        return gl.at[zz, yy, :, pl.ds(starts[i] + which * shares[i], shares[i])]

    def wo_at(slab, block, h):
        rows = pl.ds(pl.multiple_of(block * part, 128), part)
        return wo.at[slab, rows, pl.ds(h * wide, wide)]

    def out_rows(to, h):
        return out_w.at[pl.ds(pl.multiple_of(to * part, 128), part), pl.ds(h * wide, wide)]

    def hid_at(b, k, i):
        return hid.at[b, :, pl.ds(pl.multiple_of(k * part + i * first_share, LANES), shares[i])]

    def cols_of(w, to, i):
        return w.at[:, pl.ds(pl.multiple_of(to * part + i * first_share, LANES), shares[i])]

    own = xn.at[col, z]
    w_slab, w_block = jnp.where(z == col, y, 2), jnp.where(z == col, col, z)
    ins = [
        pltpu.make_async_copy(tokens, own, loc.at[0]),
        pltpu.make_async_copy(out_rows(z, 0), wo_at(w_slab, w_block, 0), loc.at[1]),
        pltpu.make_async_copy(out_rows(z, 1), wo_at(w_slab, w_block, 1), loc.at[2]),
    ]
    ins += [
        pltpu.make_async_copy(cols_of(w, z, i), gl_of(z, y, i, which), loc.at[3 + 2 * i + which])
        for i in range(2)
        for which, w in enumerate((gate_w, linear_w))
    ]
    for each in ins:
        each.start()

    barrier = pltpu.get_barrier_semaphore()
    peers = [at_z(near[1]), at_z(near[2]), at_z(near[3]), at_y, at_x, at_c, at_d]
    for peer in peers:
        pl.semaphore_signal(barrier, inc=1, device_id=peer, device_id_type=MESH)

    ins[0].wait()
    piece = 64

    @pl.loop(0, size // piece)
    def _(i):
        rows = pl.ds(pl.multiple_of(i * piece, piece), piece)
        values = xn[col, z, rows, :].astype(F32)
        sums = jnp.sum(values * values, axis=-1, keepdims=True)
        ss[col, rows, :] = jnp.broadcast_to(sums, (piece, LANES))

    pl.semaphore_wait(barrier, len(peers))

    def g_send(m, i):
        to = near[m]
        for which, w in enumerate((gate_w, linear_w)):
            copy(
                cols_of(w, to, i), gl_of(z, y, i, which), g_zs.at[m, i], g_z.at[z, i], at_z(to)
            ).start()

    def g_pass(zz, i):
        ref = gl_at(zz, y, i)
        copy(ref, ref, g_ys.at[zz, i], g_y.at[zz, i], at_y).start()

    def g_took(zz, i):
        arrived(gl_at(zz, y, i), g_z.at[zz, i])
        g_pass(zz, i)

    g_send(1, 0)
    pl.when(inner)(lambda: g_send(2, 0))
    for n, peer in enumerate((at_x, at_c, at_d)):
        copy(ss.at[col], ss.at[col], ss_s.at[n], ss_r.at[col], peer).start()
    for i in range(2):
        for which in range(2):
            ins[3 + 2 * i + which].wait()
        g_pass(z, i)
    for k in (xcol, ccol, dcol):
        arrived(ss.at[k], ss_r.at[k])

    @pl.loop(0, size // piece)
    def _(i):
        rows = pl.ds(pl.multiple_of(i * piece, piece), piece)
        total = ss[0, rows, :]
        for k in range(1, zs):
            total = total + ss[k, rows, :]
        scale = lax.rsqrt(total * (1.0 / features) + 1e-06)
        scale = jnp.concatenate([scale] * (width // LANES), axis=1)
        values = xn[col, z, rows, :].astype(F32) * scale * gain[...].astype(F32)
        xn[col, z, rows, :] = values.astype(BF16)

    def t_right(b):
        copy(xn.at[col, b], xn.at[col, b], t_zr.at[b], t_r.at[col, b], at_z(z + 1)).start()

    def t_left(b):
        copy(xn.at[col, b], xn.at[col, b], t_zl.at[b], t_r.at[col, b], at_z(z - 1)).start()

    def t_col(b):
        copy(xn.at[col, b], xn.at[col, b], t_x.at[b], t_r.at[col, b], at_x).start()
        copy(xn.at[col, b], xn.at[col, b], t_c.at[b], t_r.at[col, b], at_c).start()

    def t_over(b):
        arrived(xn.at[xcol, b], t_r.at[xcol, b])
        copy(xn.at[xcol, b], xn.at[xcol, b], t_d.at[b], t_r.at[xcol, b], at_c).start()

    def w_place(zz):
        return jnp.where(zz == col, y, 2), jnp.where(zz == col, col, zz)

    def w_out(m, h):
        zz = near[m]
        ref = wo_at(*w_place(zz), h)

        @pl.when(zz == col)
        def _():
            copy(ref, ref, w_ys.at[col, h], w_y.at[col, h], at_y).start()

        @pl.when(zz != col)
        def _():
            copy(ref, wo_at(y, col, h), w_xs.at[m, h], w_x.at[col, h], (row, zz)).start()

    def w_send(m, h):
        to = near[m]
        copy(out_rows(to, h), wo_at(w_slab, w_block, h), w_zs.at[m, h], w_z.at[z, h], at_z(to)).start()

    def w_took(m, h):
        arrived(wo_at(*w_place(near[m]), h), w_z.at[near[m], h])
        w_out(m, h)

    def w_over(p, h):
        arrived(wo_at(y, p, h), w_x.at[p, h])
        copy(wo_at(y, p, h), wo_at(y, p, h), w_ys.at[p, h], w_y.at[p, h], at_y).start()

    def t_step(s):
        below, above = z >= s, z + s < zs

        def from_below():
            arrived(xn.at[col, z - s], t_r.at[col, z - s])
            pl.when(z < zs - 1)(lambda: t_right(z - s))

        def from_above():
            arrived(xn.at[col, z + s], t_r.at[col, z + s])
            pl.when(z > 0)(lambda: t_left(z + s))

        pl.when(below & (z < zs // 2))(from_below)
        pl.when(above)(from_above)
        pl.when(below & (z >= zs // 2))(from_below)
        pl.when(below)(lambda: t_col(z - s))
        pl.when(above)(lambda: t_col(z + s))

    def t_over_step(s):
        pl.when(z >= s)(lambda: t_over(z - s))
        pl.when(z + s < zs)(lambda: t_over(z + s))

    far_outer = ((3, 0), (2, 0), (3, 1), (2, 1))

    def both(on_inner, on_outer):
        pl.when(inner)(on_inner)
        pl.when(outer)(on_outer)

    def stage(k, pieces):
        if 0 < k <= len(pieces):
            m, i = pieces[k - 1]
            left_here(gl_at(z, y, i), g_zs.at[m, i])
        for n in (0, 1) if k == 0 else (k + 1,):
            if n < len(pieces):
                g_send(*pieces[n])

    def near_out():
        for h in range(2):
            w_send(1, h)

    def w_stage(h):
        if h:
            for m in (2, 3):
                left_here(wo_at(w_slab, w_block, 0), w_zs.at[m, 0])

        def on(order):
            for m in order:
                w_send(m, h)

        both(lambda: on((2, 3) if h else (3,)), lambda: on((3, 2)))

    pl.when(z < zs - 1)(lambda: t_right(z))
    pl.when(z > 0)(lambda: t_left(z))
    t_col(z)
    pl.when(outer)(lambda: g_send(1, 1))
    third = jnp.where(inner, near[2], near[3])
    last = jnp.where(inner, near[3], near[2])
    g_took(near[1], 0)
    t_step(1)

    def early():
        g_took(third, 0)
        g_took(near[1], 1)

    pl.when(inner)(early)
    t_step(2)

    def relayed(up, b):
        left_here(xn.at[col, b], (t_zr if up else t_zl).at[b])

    lower, upper = inner & (z < zs // 2), inner & (z >= zs // 2)
    pl.when(lower)(lambda: relayed(True, z - 1))
    pl.when(upper)(lambda: relayed(False, z + 1))
    @pl.when(inner)
    def _():
        g_send(2, 1)
        w_send(2, 0)

    t_step(3)
    pl.when(outer)(lambda: stage(0, far_outer))
    t_over(z)
    t_over_step(1)

    @pl.when(lower)
    def _():
        relayed(False, z + 1)
        relayed(False, z + 2)

    @pl.when(upper)
    def _():
        relayed(True, z - 1)
        relayed(True, z - 2)

    @pl.when(inner)
    def _():
        g_send(1, 1)
        g_send(3, 0)
        g_took(third, 1)

    t_over_step(2)
    t_over_step(3)
    for h in range(2):
        ins[1 + h].wait()
        w_out(0, h)

    tile = 2 * LANES
    tiles = 2 * part // tile
    depth = gl.shape[2]

    def product(kk, b, n, yys):
        lanes = pl.ds(pl.multiple_of(n * tile, tile), tile)
        value = None
        for yy in yys:
            columns = pl.ds(pl.multiple_of(yy * depth, depth), depth)
            term = dot(xn[kk, b, :, columns], gl[kk, yy, :, lanes])
            value = term if value is None else value + term
        return value, lanes

    def inputs(kk, i, first, yys, block=None):
        count = 2 * shares[i] // tile

        @pl.loop(0, count if block is not None else zs * count)
        def _(n):
            b, at = (n // count, n % count) if block is None else (block, n)
            value, lanes = product(kk, b, starts[i] // tile + at, yys)
            if first:
                acc[b, :, lanes] = value
            else:
                acc[b, :, lanes] = acc[b, :, lanes] + value

    def gl_whole(zz, i):
        arrived(gl_at(zz, 1 - y, i), g_y.at[zz, i])

    cut = 64

    def h_send(j, i):
        b = blocks[j]
        copy(hid_at(b, col, i), hid_at(b, col, i), h_x.at[j, i], h_r.at[col, b, i], at_x).start()
        copy(hid_at(b, col, i), hid_at(b, col, i), h_c.at[j, i], h_r.at[col, b, i], at_c).start()

    def h_over(j, i):
        b = blocks[j]
        arrived(hid_at(b, xcol, i), h_r.at[xcol, b, i])
        copy(hid_at(b, xcol, i), hid_at(b, xcol, i), h_d.at[j, i], h_r.at[xcol, b, i], at_c).start()

    def hidden(j, i):
        b = blocks[j]

        @pl.loop(0, size // cut)
        def _(n):
            rows = pl.ds(pl.multiple_of(n * cut, cut), cut)
            gate = acc[b, rows, pl.ds(starts[i], shares[i])]
            linear = acc[b, rows, pl.ds(starts[i] + shares[i], shares[i])]
            value = (jax.nn.gelu(gate, approximate=True) * linear).astype(BF16)
            hid[b, rows, pl.ds(pl.multiple_of(col * part + i * first_share, LANES), shares[i])] = value

    orders = [sorted(range(zs), key=lambda b, at=at: -abs(b - at)) for at in range(zs)]
    blocks = [pick(z, [order[j] for order in orders]) for j in range(zs)]

    for b in range(zs):
        for k in (ccol, dcol):
            arrived(xn.at[k, b], t_r.at[k, b])
    gl_whole(z, 0)
    inputs(z, 0, True, (0, 1))

    @pl.when(inner)
    def _():
        g_send(3, 1)
        g_took(last, 0)

    pl.when(outer)(lambda: stage(1, far_outer))
    near_out()
    gl_whole(near[1], 0)
    inputs(near[1], 0, False, (0, 1))

    @pl.when(outer)
    def _():
        g_took(near[1], 1)
        g_took(third, 0)

    gl_whole(z, 1)
    inputs(z, 1, True, (0, 1))

    @pl.when(outer)
    def _():
        stage(2, far_outer)
        g_took(last, 0)

    gl_whole(near[1], 1)
    inputs(near[1], 1, False, (0, 1))
    gl_whole(third, 0)
    inputs(third, 0, False, (0, 1))
    pl.when(outer)(lambda: g_took(third, 1))
    gl_whole(last, 0)
    for j in range(zs):
        inputs(last, 0, False, (0, 1), blocks[j])
        hidden(j, 0)
        h_send(j, 0)
    pl.when(outer)(lambda: stage(3, far_outer))
    pl.when(inner)(lambda: g_took(last, 1))
    gl_whole(third, 1)
    inputs(third, 1, False, (0, 1))

    def inner_left():
        for m, i in ((2, 1), (3, 0), (3, 1)):
            left_here(gl_at(z, y, i), g_zs.at[m, i])

    both(inner_left, lambda: stage(4, far_outer))
    w_stage(0)
    pl.when(outer)(lambda: g_took(last, 1))
    inputs(last, 1, False, (y,))
    gl_whole(last, 1)
    for j in range(zs):
        inputs(last, 1, False, (1 - y,), blocks[j])
        hidden(j, 1)
        if j < 2:
            h_send(j, 1)

    for b in range(zs):
        left_here(xn.at[col, b], t_x.at[b])
        left_here(xn.at[col, b], t_c.at[b])
        left_here(xn.at[xcol, b], t_d.at[b])

        @pl.when((b <= z) & (z < zs - 1) & (outer | (b == z)))
        def _(b=b):
            left_here(xn.at[col, b], t_zr.at[b])

        @pl.when((b >= z) & (z > 0) & (outer | (b == z)))
        def _(b=b):
            left_here(xn.at[col, b], t_zl.at[b])

    @pl.when(z > 0)
    def _():
        pl.semaphore_signal(credit.at[0], inc=1, device_id=at_z(z - 1), device_id_type=MESH)

    @pl.when(z < zs - 1)
    def _():
        pl.semaphore_signal(credit.at[1], inc=1, device_id=at_z(z + 1), device_id_type=MESH)

    def outputs(h, j):
        b = blocks[j]

        @pl.loop(0, 2)
        def _(yy):
            value = dot(hid[b], wo[yy, :, pl.ds(h * wide, wide)])
            acc[b, :, pl.ds(pl.multiple_of(h * outw + yy * wide, wide), wide)] = value

    def half_of(slot, b, h):
        return xn.at[slot, b, :, pl.ds(h * outw, outw)]

    def carries(h, b):
        from_left = (b >= z) & (z > 0)
        from_right = (b <= z) & (z < zs - 1)
        slot = jnp.where(b == z, 2, 0)
        pl.when(from_left)(lambda: arrived(half_of(0, b, h), o_r.at[0, b, h]))
        pl.when(from_right)(lambda: arrived(half_of(slot, b, h), o_r.at[1, b, h]))
        return from_left, from_right

    def relay(h, j):
        b = blocks[j]
        from_left, from_right = carries(h, b)
        lanes = pl.ds(h * outw, outw)
        carry = from_left | from_right

        @pl.loop(0, size // cut)
        def _(i):
            rows = pl.ds(pl.multiple_of(i * cut, cut), cut)
            value = acc[b, rows, lanes] + jnp.where(carry, xn[0, b, rows, lanes].astype(F32), 0.0)
            xn[1, b, rows, lanes] = value.astype(BF16)

        @pl.when(b > z)
        def _():
            copy(half_of(1, b, h), half_of(0, b, h), o_s.at[j, h], o_r.at[0, b, h], at_z(z + 1)).start()

        @pl.when(b < z)
        def _():
            slot = jnp.where(b == z - 1, 2, 0)
            copy(half_of(1, b, h), half_of(slot, b, h), o_s.at[j, h], o_r.at[1, b, h], at_z(z - 1)).start()

    def finish(h):
        from_left, from_right = carries(h, z)

        @pl.loop(0, size // cut)
        def _(i):
            rows = pl.ds(pl.multiple_of(i * cut, cut), cut)
            for yy in range(2):
                lanes = pl.ds(h * outw + yy * wide, wide)
                value = acc[z, rows, lanes]
                value = value + jnp.where(from_left, xn[0, z, rows, lanes].astype(F32), 0.0)
                value = value + jnp.where(from_right, xn[2, z, rows, lanes].astype(F32), 0.0)
                out[rows, pl.ds(yy * outw + h * wide, wide)] = value.astype(BF16)

    def hid_whole(j):
        for k in (ccol, dcol):
            for i in range(2):
                arrived(hid_at(blocks[j], k, i), h_r.at[k, blocks[j], i])

    def wo_whole(h):
        for p in range(zs):
            arrived(wo_at(1 - y, p, h), w_y.at[p, h])

    w_stage(1)
    for m in range(1, zs):
        w_took(m, 0)
    h_send(2, 1)
    h_send(3, 1)
    for j in range(zs):
        h_over(j, 0)
    h_over(0, 1)
    h_over(1, 1)
    for p in (ccol, xcol, dcol):
        w_over(p, 0)
    for m in range(1, zs):
        w_took(m, 1)
    wo_whole(0)
    hid_whole(0)
    outputs(0, 0)
    pl.when(z < zs - 1)(lambda: pl.semaphore_wait(credit.at[0], 1))
    pl.when(z > 0)(lambda: pl.semaphore_wait(credit.at[1], 1))
    pl.when(outer)(lambda: relay(0, 0))
    hid_whole(1)
    outputs(0, 1)
    pl.when(outer)(lambda: relay(0, 1))
    for p in (ccol, xcol, dcol):
        w_over(p, 1)
    h_over(2, 1)
    h_over(3, 1)
    hid_whole(2)
    outputs(0, 2)
    both(lambda: relay(0, 0), lambda: relay(0, 2))
    pl.when(inner)(lambda: relay(0, 1))
    pl.when(inner)(lambda: relay(0, 2))
    wo_whole(1)
    for j in range(zs - 1):
        outputs(1, j)
        relay(1, j)
    hid_whole(3)
    for h in range(2):
        outputs(h, zs - 1)
    for h in range(2):
        finish(h)

    for n in range(3):
        left_here(ss.at[col], ss_s.at[n])
    pl.when(inner)(lambda: left_here(gl_at(z, y, 0), g_zs.at[2, 0]))
    for m in range(zs):
        for i in range(2):
            if m == 1:
                left_here(gl_at(z, y, i), g_zs.at[m, i])
            left_here(gl_at(m, y, i), g_ys.at[m, i])
        for h in range(2):
            if m == 1 or m and h:
                left_here(wo_at(w_slab, w_block, h), w_zs.at[m, h])
            pl.when(near[m] != col)(lambda m=m, h=h: left_here(wo_at(y, col, h), w_xs.at[m, h]))
            left_here(wo_at(y, m, h), w_ys.at[m, h])
    for j in range(zs):
        for i in range(2):
            for sem in (h_x, h_c, h_d):
                left_here(hid_at(blocks[j], col, i), sem.at[j, i])
        if j < zs - 1:
            for h in range(2):
                left_here(half_of(1, blocks[j], h), o_s.at[j, h])


def scratch_of(zs, size, width, depth, part, outw):
    cols = zs
    dma = pltpu.SemaphoreType.DMA
    buffers = [
        ((cols, zs, size, width), BF16),
        ((zs, 2, depth, 2 * part), BF16),
        ((zs, size, 2 * part), F32),
        ((zs, size, cols * part), BF16),
        ((3, cols * part, outw), BF16),
        ((cols, size, LANES), F32),
    ]
    sems = [
        (7,), (3,), (cols,), (cols, zs), (zs,), (zs,), (zs,), (zs,), (zs,), (zs, 2), (zs, 2), (zs, 2), (zs, 2),
        (zs, 2), (zs, 2), (cols, 2), (zs, 2), (cols, 2), (cols, 2), (cols, zs, 2), (zs, 2), (zs, 2), (zs, 2), (2, zs, 2),
        (zs, 2),
    ]
    return buffers, [dma(s) for s in sems] + [pltpu.SemaphoreType.REGULAR((2,))]


def fused(zs, buffers, sems, tokens, norm_gain, gate_weight, linear_weight, output_weight):
    anywhere = pl.BlockSpec(memory_space=pl.ANY)
    vmem = pl.BlockSpec(memory_space=pltpu.VMEM)
    return pl.pallas_call(
        functools.partial(body, zs),
        out_shape=jax.ShapeDtypeStruct(tokens.shape, BF16),
        in_specs=[anywhere, vmem, anywhere, anywhere, anywhere],
        out_specs=vmem,
        scratch_shapes=[pltpu.VMEM(shape, kind) for shape, kind in buffers] + sems,
        compiler_params=pltpu.CompilerParams(
            collective_id=0, has_side_effects=True, vmem_limit_bytes=VMEM_LIMIT
        ),
        name="ffn",
    )(tokens, norm_gain.reshape(1, -1), gate_weight, linear_weight, output_weight)


def solution(mesh):
    rows, cols = mesh.shape["row"], mesh.shape["col"]
    zs, xs = rows // 2, cols // 2

    def local(tokens, norm_gain, gate_weight, linear_weight, output_weight):
        args = (tokens, norm_gain, gate_weight, linear_weight, output_weight)
        size, width = tokens.shape
        depth, units = gate_weight.shape
        outw = output_weight.shape[1]
        part = units // zs
        fits = xs == 2 and zs == cols == 4 and units % (zs * LANES) == 0
        fits = fits and 2 * depth == width and 2 * outw == width and outw % (2 * LANES) == 0
        fits = fits and size % 64 == 0
        if fits:
            buffers, sems = scratch_of(zs, size, width, depth, part, outw)
            held = sum(functools.reduce(lambda a, b: a * b, s) * jnp.dtype(k).itemsize for s, k in buffers)
            if held <= SCRATCH_MOST:
                return fused(zs, buffers, sems, *args)
        return gathered(*args)

    return jax.shard_map(
        local,
        mesh=mesh,
        in_specs=(P("row", "col"), P("col"), P("row", "col"), P("row", "col"), P("col", "row")),
        out_specs=P("row", "col"),
        check_vma=False,
    )
```
